32 devices in a mesh: blk: 16 (over z, x, core), cuts: 2 (over y).
Axes of the slice: x: 2, y: 2, z: 4, core: 2. Of those that a mesh axis runs over, the one named last changes fastest.
Arguments:
- left_env: bfloat16 [2048, 8, 2048], P('blk', 'cuts'), may hold values from -4 to 4
- right_env: bfloat16 [2048, 8, 2048], P('blk', 'cuts'), may hold values from -4 to 4
- left_core: float32 [8, 8, 2, 2], replicated, may hold values from -1.5 to 1.5
- right_core: float32 [8, 8, 2, 2], replicated, may hold values from -1.5 to 1.5
- slot_bond: int32 [8], replicated, may hold values from 0 to 7, each once
- krylov_basis: float32 [8, 2048, 4, 2048], P(None, 'blk', None, 'cuts'), may hold values from -30 to 30
- beta_prev: float32 [], replicated, may hold values from 0.3 to 1.2
Outputs:
- next_vector: float32 [2048, 4, 2048], P('blk', None, 'cuts')
- alpha_values: float32 [1], replicated
- beta_values: float32 [1], replicated
The draws below stay inside these ranges and needn't reach their ends.
Inputs may be any that keep to these rules, and one draw needn't show every extreme that they name: `slot_bond`: a permutation of the 8 bond values.
All inputs are finite; a program needn't handle non-finite values.
Results may differ from the reference program's by a relative error of at most 0.00073.
The reference program's roundings to bfloat16 on the way (of `current` and `mixed_left`) count: a program that leaves them out, or rounds other values in their place, can miss the bound.
Values may be sent and summed in bfloat16 or wider, within the bound.
A program may use at most 192 MiB of HBM per device.

```python
import math
import jax
import jax.numpy as jnp
from jax import lax

D = 2048
PHYS = 2
W = 8
KRY = 8
STEPS = 1


def draw_environment(key):
    key_noise, key_diag = jax.random.split(key, 2)
    noise_part = jnp.clip(jax.random.normal(key_noise, (D, W, D), jnp.float32), -6.0, 6.0) * (0.8 / math.sqrt(D))
    diag_values = jax.random.uniform(key_diag, (D, W), jnp.float32, 0.5, 1.5)
    on_diagonal = jnp.arange(D, dtype=jnp.int32)[:, None, None] == jnp.arange(D, dtype=jnp.int32)[None, None, :]
    return (noise_part + jnp.where(on_diagonal, diag_values[:, :, None], 0.0)).astype(jnp.bfloat16)


def draw_left_env(key, part):
    return draw_environment(jax.random.fold_in(key, 11))


def draw_right_env(key, part):
    return draw_environment(jax.random.fold_in(key, 23))


def draw_krylov_basis(key, part):
    key_common, key_single = jax.random.split(jax.random.fold_in(key, 37), 2)
    one_shape = (D, PHYS * PHYS, D)
    rising_scale = jnp.exp(math.log(3.0) * jnp.arange(D, dtype=jnp.float32) / D)[:, None, None]
    common = jnp.clip(jax.random.normal(key_common, one_shape, jnp.float32), -6.0, 6.0)
    single = jnp.clip(jax.random.normal(key_single, (KRY,) + one_shape, jnp.float32), -6.0, 6.0)
    return rising_scale[None] * (0.6 * common[None] + 0.8 * single)


def bell_draw(own_key, shape, scale, bound, kind=jnp.bfloat16):
    values = scale * jax.random.normal(own_key, shape, jnp.float32)
    return jnp.clip(values, min=-bound, max=bound).astype(kind)


def setup_inputs(seed: int = 0) -> dict:
    streams_of = jax.random.split(jax.random.key(seed), 8)
    left_env = draw_left_env(jax.random.fold_in(streams_of[7], 71), 0)
    right_env = draw_right_env(jax.random.fold_in(streams_of[7], 71), 0)
    left_core = bell_draw(streams_of[2], (W, W, PHYS, PHYS), (W * PHYS) ** -0.5, 1.5, jnp.float32)
    right_core = bell_draw(streams_of[3], (W, W, PHYS, PHYS), (W * PHYS) ** -0.5, 1.5, jnp.float32)
    slot_bond = jax.random.permutation(streams_of[4], W).astype(jnp.int32)
    krylov_basis = draw_krylov_basis(jax.random.fold_in(streams_of[7], 71), 0)
    beta_prev = jnp.clip(jax.random.uniform(streams_of[6], (), jnp.float32, 0.3, 1.2), 0.3, 1.2)
    return dict(left_env=left_env, right_env=right_env, left_core=left_core, right_core=right_core, slot_bond=slot_bond, krylov_basis=krylov_basis, beta_prev=beta_prev)


def build_table(left_core, right_core, slot_bond):
    picked = left_core[slot_bond]
    table = jnp.einsum('kxac,xybd->kyabcd', picked, right_core, precision=lax.Precision.HIGHEST)
    return table.reshape(W, W, PHYS * PHYS, PHYS * PHYS)

def apply_hamiltonian(left_env, right_env, mpo_table, current):
    pair_count = PHYS * PHYS
    block_rows = min(D, 256)
    block_count = D // block_rows
    right_matrix = right_env.reshape(D, W * D).T
    vector_matrix = current.reshape(D, pair_count * D)

    def one_block(block_index):
        start_row = (block_index * block_rows).astype(jnp.int32)
        left_rows = lax.dynamic_slice_in_dim(left_env, start_row, block_rows, 0).reshape(block_rows * W, D)
        projected = jnp.dot(left_rows, vector_matrix, preferred_element_type=jnp.float32)
        projected = projected.reshape(block_rows, W, pair_count, D)
        mixed_left = jnp.einsum('kypq,akqb->apyb', mpo_table, projected, precision=lax.Precision.HIGHEST).astype(jnp.bfloat16)
        image_rows = jnp.dot(mixed_left.reshape(block_rows * pair_count, W * D), right_matrix, preferred_element_type=jnp.float32)
        return image_rows.reshape(block_rows, pair_count, D)
    image_vec = lax.map(one_block, jnp.arange(block_count, dtype=jnp.int32))
    return image_vec.reshape(D, pair_count, D)

def reference(left_env, right_env, left_core, right_core, slot_bond, krylov_basis, beta_prev):
    highest = lax.Precision.HIGHEST
    entries = float(D * PHYS * PHYS * D)
    mpo_table = build_table(left_core, right_core, slot_bond)
    basis_now = krylov_basis
    beta_now = beta_prev
    alpha_list = []
    beta_list = []
    next_vector = krylov_basis[KRY - 1]
    for step_index in range(STEPS):
        current_f = basis_now[KRY - 1]
        previous = basis_now[KRY - 2]
        image_vec = apply_hamiltonian(left_env, right_env, mpo_table, current_f.astype(jnp.bfloat16))
        alpha_now = jnp.sum(current_f * image_vec) / entries
        first_pass = image_vec - alpha_now * current_f - beta_now * previous
        ortho_coeffs = jnp.einsum('japb,apb->j', basis_now, first_pass, precision=highest) / entries
        second_pass = first_pass - jnp.einsum('j,japb->apb', ortho_coeffs, basis_now, precision=highest)
        beta_new = jnp.sqrt(jnp.sum(second_pass * second_pass) / entries + 1e-06)
        next_vector = second_pass / beta_new
        alpha_list.append(alpha_now)
        beta_list.append(beta_new)
        basis_now = jnp.concatenate([basis_now[1:], next_vector[None]], axis=0)
        beta_now = beta_new
    return (next_vector, jnp.stack(alpha_list), jnp.stack(beta_list))
```

```python
import functools

import jax
import jax.numpy as jnp
from jax import lax
from jax.experimental import pallas as pl
from jax.experimental.pallas import tpu as pltpu
from jax.sharding import PartitionSpec as P

VMEM_BYTES = 60 * 1024 * 1024


def params():
    return pltpu.CompilerParams(vmem_limit_bytes=VMEM_BYTES)


def tile_of(size, most):
    return most if size % most == 0 else size


def build_table(left_core, right_core, slot_bond):
    bond_width = left_core.shape[0]
    phys_dim = left_core.shape[2]
    chosen = (slot_bond[:, None] == jnp.arange(bond_width, dtype=jnp.int32)[None, :]).astype(
        jnp.float32
    )
    picked = jnp.einsum("kw,wxac->kxac", chosen, left_core, precision=lax.Precision.HIGHEST)
    table = jnp.einsum("kxac,xybd->kyabcd", picked, right_core, precision=lax.Precision.HIGHEST)
    return table.reshape(bond_width, bond_width, phys_dim * phys_dim, phys_dim * phys_dim)


def mix_kernel(mix_ref, left_ref, cur_ref, out_ref, proj):
    slots, rows, depth = left_ref.shape
    pairs = cur_ref.shape[0]
    bonds = out_ref.shape[0]
    cols = cur_ref.shape[2]

    @pl.loop(0, pairs)
    def _(q):
        proj[q] = jnp.dot(
            left_ref[...].reshape(slots * rows, depth),
            cur_ref[q],
            preferred_element_type=jnp.float32,
        ).reshape(slots, rows, cols)

    @pl.loop(0, rows // 16)
    def _(g):
        mixed = []
        for h in range(2):
            at = pl.ds(pl.multiple_of(g * 16 + h * 8, 8), 8)
            stacked = jnp.concatenate(
                [proj[q, k, at, :] for k in range(slots) for q in range(pairs)], axis=0
            )
            mixed.append(
                jnp.dot(
                    mix_ref[...],
                    stacked,
                    precision=lax.Precision.HIGHEST,
                    preferred_element_type=jnp.float32,
                )
            )
        at = pl.ds(pl.multiple_of(g * 16, 16), 16)
        for y in range(bonds):
            for p in range(pairs):
                i = (y * pairs + p) * 8
                out_ref[y, p, at, :] = jnp.concatenate(
                    [m[i : i + 8] for m in mixed], axis=0
                ).astype(out_ref.dtype)


def mixed_left_of(table, left_k, cur_full):
    slots, rows, depth = left_k.shape
    pairs, _, cols = cur_full.shape
    bonds = table.shape[1]
    tb = tile_of(cols, 256)
    square = table.transpose(1, 2, 0, 3).reshape(bonds * pairs, slots * pairs)
    mix = jnp.kron(square, jnp.eye(8, dtype=jnp.float32))
    return pl.pallas_call(
        mix_kernel,
        grid=(cols // tb,),
        in_specs=[
            pl.BlockSpec(mix.shape, lambda i: (0, 0)),
            pl.BlockSpec((slots, rows, depth), lambda i: (0, 0, 0)),
            pl.BlockSpec((pairs, depth, tb), lambda i: (0, 0, i)),
        ],
        out_specs=pl.BlockSpec((bonds, pairs, rows, tb), lambda i: (0, 0, 0, i)),
        out_shape=jax.ShapeDtypeStruct((bonds, pairs, rows, cols), jnp.bfloat16),
        scratch_shapes=[pltpu.VMEM((pairs, slots, rows, tb), jnp.float32)],
        compiler_params=params(),
        cost_estimate=pl.CostEstimate(
            flops=2 * slots * rows * depth * pairs * cols,
            bytes_accessed=2 * (left_k.size + cur_full.size + bonds * pairs * rows * cols),
            transcendentals=0,
        ),
    )(mix, left_k, cur_full)


def image_kernel(start_ref, mixed_ref, right_ref, out_ref):
    bonds = mixed_ref.shape[0]
    out_ref[...] = jnp.zeros_like(out_ref)

    @pl.loop(0, bonds)
    def _(y):
        out_ref[...] += lax.dot_general(
            mixed_ref[y],
            right_ref[y],
            (((1,), (1,)), ((), ())),
            preferred_element_type=jnp.float32,
        )


def image_part(mixed, right_full, start, count):
    bonds, lines, cols = mixed.shape
    tb = tile_of(count, 256)
    return pl.pallas_call(
        image_kernel,
        grid_spec=pltpu.PrefetchScalarGridSpec(
            num_scalar_prefetch=1,
            grid=(count // tb,),
            in_specs=[
                pl.BlockSpec((bonds, lines, cols), lambda i, s: (0, 0, 0)),
                pl.BlockSpec((bonds, tb, cols), lambda i, s: (0, s[0] + i, 0)),
            ],
            out_specs=pl.BlockSpec((lines, tb), lambda i, s: (0, i)),
        ),
        out_shape=jax.ShapeDtypeStruct((lines, count), jnp.float32),
        compiler_params=params(),
        cost_estimate=pl.CostEstimate(
            flops=2 * bonds * lines * cols * count,
            bytes_accessed=2 * (mixed.size + bonds * count * cols),
            transcendentals=0,
        ),
    )((start // tb).reshape(1).astype(jnp.int32), mixed, right_full)


def gram_kernel(basis_ref, out_ref):
    basis_count, rows, pairs, cols = basis_ref.shape
    chunk = 4
    lanes = cols // 128

    @pl.when(pl.program_id(0) == 0)
    def _():
        out_ref[...] = jnp.zeros_like(out_ref)

    @pl.loop(0, rows // chunk)
    def _(r):
        for c in range(lanes):
            vecs = [
                basis_ref[j, pl.ds(r * chunk, chunk), :, c * 128 : (c + 1) * 128]
                for j in range(basis_count)
            ]
            i = 0
            for j in range(basis_count):
                for k in range(j, basis_count):
                    out_ref[i] += jnp.sum(vecs[j] * vecs[k], axis=0)
                    i += 1


def gram_of(basis):
    basis_count, rows, pairs, cols = basis.shape
    count = basis_count * (basis_count + 1) // 2
    ta = tile_of(rows, 16)
    sums = pl.pallas_call(
        gram_kernel,
        grid=(rows // ta,),
        in_specs=[pl.BlockSpec((basis_count, ta, pairs, cols), lambda i: (0, i, 0, 0))],
        out_specs=pl.BlockSpec((count, pairs, 128), lambda i: (0, 0, 0)),
        out_shape=jax.ShapeDtypeStruct((count, pairs, 128), jnp.float32),
        compiler_params=params(),
        cost_estimate=pl.CostEstimate(
            flops=2 * count * rows * pairs * cols,
            bytes_accessed=4 * basis.size,
            transcendentals=0,
        ),
    )(basis)
    return jnp.sum(sums, axis=(1, 2))


def dots_kernel(basis_ref, image_ref, out_ref):
    basis_count, rows, pairs, cols = basis_ref.shape

    @pl.when(pl.program_id(0) == 0)
    def _():
        out_ref[...] = jnp.zeros_like(out_ref)

    for c in range(cols // 128):
        at = slice(c * 128, (c + 1) * 128)
        image = image_ref[:, :, at]
        for j in range(basis_count):
            out_ref[j] += jnp.sum(basis_ref[j, :, :, at] * image, axis=0)
        out_ref[basis_count] += jnp.sum(image * image, axis=0)


def dots_of(basis, image):
    basis_count, rows, pairs, cols = basis.shape
    ta = tile_of(rows, 16)
    sums = pl.pallas_call(
        dots_kernel,
        grid=(rows // ta,),
        in_specs=[
            pl.BlockSpec((basis_count, ta, pairs, cols), lambda i: (0, i, 0, 0)),
            pl.BlockSpec((ta, pairs, cols), lambda i: (i, 0, 0)),
        ],
        out_specs=pl.BlockSpec((basis_count + 1, pairs, 128), lambda i: (0, 0, 0)),
        out_shape=jax.ShapeDtypeStruct((basis_count + 1, pairs, 128), jnp.float32),
        compiler_params=params(),
    )(basis, image)
    return jnp.sum(sums, axis=(1, 2))


def final_kernel(coef_ref, basis_ref, image_ref, out_ref):
    basis_count = basis_ref.shape[0]
    total = image_ref[...]
    for j in range(basis_count):
        total = total - coef_ref[j] * basis_ref[j]
    out_ref[...] = total * coef_ref[basis_count]


def final_of(coefs, basis, image):
    basis_count, rows, pairs, cols = basis.shape
    ta = tile_of(rows, 16)
    return pl.pallas_call(
        final_kernel,
        grid=(rows // ta,),
        in_specs=[
            pl.BlockSpec(memory_space=pltpu.SMEM),
            pl.BlockSpec((basis_count, ta, pairs, cols), lambda i: (0, i, 0, 0)),
            pl.BlockSpec((ta, pairs, cols), lambda i: (i, 0, 0)),
        ],
        out_specs=pl.BlockSpec((ta, pairs, cols), lambda i: (i, 0, 0)),
        out_shape=jax.ShapeDtypeStruct((rows, pairs, cols), jnp.float32),
        compiler_params=params(),
    )(coefs, basis, image)


def on_device(
    cuts, left_env, right_env, left_core, right_core, slot_bond, krylov_basis, beta_prev
):
    bond_width = left_core.shape[0]
    pair_count = left_core.shape[2] * left_core.shape[2]
    basis_count, row_count, _, col_count = krylov_basis.shape
    full_width = left_env.shape[2]
    entries = float(full_width * pair_count * full_width)
    table = build_table(left_core, right_core, slot_bond)
    me = lax.axis_index("cuts")
    swap = [(0, 1), (1, 0)]

    current = krylov_basis[basis_count - 1].astype(jnp.bfloat16).transpose(1, 0, 2)
    left_t = left_env.transpose(1, 0, 2)
    right_t = right_env.transpose(1, 0, 2)
    if cuts == 2:
        half = left_t.shape[0]
        theirs = lax.dynamic_slice_in_dim(right_t, (1 - me) * col_count, col_count, 2)
        mine = lax.dynamic_slice_in_dim(right_t, me * col_count, col_count, 2)
        right_k = jnp.concatenate([mine, lax.ppermute(theirs, "cuts", swap)], axis=0)
        left_k = jnp.concatenate([left_t, lax.ppermute(left_t, "cuts", swap)], axis=0)
        turned = jnp.roll(jnp.roll(table, -half, axis=0), -half, axis=1)
        table = jnp.where(me == 0, table, turned)
    else:
        left_k = lax.all_gather(left_t, "cuts", axis=0, tiled=True)
        right_k = lax.all_to_all(right_t, "cuts", split_axis=2, concat_axis=0, tiled=True)
    cur_full = lax.all_gather(current, "blk", axis=1, tiled=True)
    right_full = lax.all_gather(right_k, "blk", axis=1, tiled=True)
    gram = gram_of(krylov_basis)

    mixed = mixed_left_of(table, left_k, cur_full)
    mixed = mixed.reshape(bond_width, pair_count * row_count, col_count)
    if cuts == 2:
        away = image_part(mixed, right_full, (1 - me) * col_count, col_count)
        away = lax.ppermute(away, "cuts", swap)
        here = image_part(mixed, right_full, me * col_count, col_count)
        image = here + away
    else:
        image = image_part(mixed, right_full, jnp.int32(0), full_width)
        image = lax.psum_scatter(image, "cuts", scatter_dimension=1, tiled=True)
    image = image.reshape(pair_count, row_count, col_count).transpose(1, 0, 2)

    sums = lax.psum(jnp.concatenate([gram, dots_of(krylov_basis, image)]), ("blk", "cuts"))
    sums = sums / entries
    count = basis_count * (basis_count + 1) // 2
    where = []
    for j in range(basis_count):
        for k in range(basis_count):
            low, high = min(j, k), max(j, k)
            where.append(low * basis_count - low * (low - 1) // 2 + high - low)
    gram_matrix = sums[jnp.array(where)].reshape(basis_count, basis_count)
    inner_prods = sums[count : count + basis_count]
    image_square = sums[count + basis_count]
    last, prior = basis_count - 1, basis_count - 2
    alpha_now = inner_prods[last]
    ortho_coeffs = (
        inner_prods - alpha_now * gram_matrix[:, last] - beta_prev * gram_matrix[:, prior]
    )
    first_square = (
        image_square
        - 2.0 * alpha_now * inner_prods[last]
        - 2.0 * beta_prev * inner_prods[prior]
        + alpha_now * alpha_now * gram_matrix[last, last]
        + 2.0 * alpha_now * beta_prev * gram_matrix[last, prior]
        + beta_prev * beta_prev * gram_matrix[prior, prior]
    )
    square_mean = (
        first_square
        - 2.0 * jnp.sum(ortho_coeffs * ortho_coeffs)
        + jnp.sum(ortho_coeffs[:, None] * gram_matrix * ortho_coeffs[None, :])
    )
    beta_new = jnp.sqrt(square_mean + 1e-06)
    index = jnp.arange(basis_count)
    coefs = (
        ortho_coeffs
        + jnp.where(index == last, alpha_now, 0.0)
        + jnp.where(index == prior, beta_prev, 0.0)
    )
    coefs = jnp.concatenate([coefs, (1.0 / beta_new)[None]])
    next_vector = final_of(coefs, krylov_basis, image)
    return (next_vector, alpha_now[None], beta_new[None])


def solution(mesh):
    in_specs = (
        P("blk", "cuts", None),
        P("blk", "cuts", None),
        P(),
        P(),
        P(),
        P(None, "blk", None, "cuts"),
        P(),
    )
    out_specs = (P("blk", None, "cuts"), P(), P())
    return jax.shard_map(
        functools.partial(on_device, mesh.shape["cuts"]),
        mesh=mesh,
        in_specs=in_specs,
        out_specs=out_specs,
        check_vma=False,
    )
```
